512 devices in a mesh: gx: 16 (over y_lo, x, core), gy: 32 (over y_hi, z).
Axes of the slice: x: 4, y: 4 (y_hi: 2, y_lo: 2; y = y_hi * 2 + y_lo), z: 16, core: 2. Of those that a mesh axis runs over, the one named last changes fastest.
Arguments:
- sources: float32 [32, 16, 256, 1024], P('gy', 'gx'), may hold values from -6 to 6
- coeff_in: bfloat16 [32, 16, 256, 256], P('gy', 'gx'), may hold values from -0.375 to 0.375
- transfer: bfloat16 [8, 32, 16, 256, 512], P(None, 'gy', 'gx'), may hold values from -0.25 to 0.25
- coeff_out: bfloat16 [32, 16, 256, 256], P('gy', 'gx'), may hold values from -0.375 to 0.375
Outputs:
- targets: float32 [32, 16, 256, 1024], P('gy', 'gx')
The draws below stay inside these ranges and needn't reach their ends.
All inputs are finite; a program needn't handle non-finite values.
Results may differ from the reference program's by a relative error of at most 0.015.
Values may be sent and summed in bfloat16 or wider, within the bound.
No kernel may reach another device: no remote copies, remote signals or barrier semaphores. Data moves between devices by JAX's collectives and lax.ppermute only.
A program may use at most 64 MiB of HBM per device.

```python
import jax
import jax.numpy as jnp
from jax import lax

RANK = 256
LEAF = 256
COLS = 1024
LEVELS = 8
N_GX = 16
N_GY = 32


def level_of(key, shape, pieces, smallest, top_value):
    def one(dim, shards_of):
        heights = jax.random.uniform(jax.random.fold_in(jax.random.fold_in(key, 6), dim), (shards_of,), jnp.float32, smallest / len(pieces), top_value / len(pieces))
        return jnp.repeat(jnp.exp(heights), shape[dim] // shards_of).reshape((-1,) + (1,) * (len(shape) - dim - 1))

    factor_of = one(*pieces[0])
    for cut in pieces[1:]:
        factor_of = factor_of * one(*cut)
    return factor_of


def noise(stream_key, dims, width, most, pieces=(), held_as=jnp.bfloat16):
    loudness = level_of(stream_key, dims, pieces, -0.22, 0.18) if pieces else 1.0
    entries = jax.random.normal(stream_key, dims, jnp.float32) * width * loudness
    return jnp.minimum(jnp.maximum(entries, -most), most).astype(held_as)


def setup_inputs(seed: int = 0) -> dict:
    key_list = jax.random.split(jax.random.key(seed), 5)
    sources = noise(key_list[0], (N_GY, N_GX, LEAF, COLS), 1.0, 6.0, ((0, 32), (1, 16)), jnp.float32)
    coeff_in = noise(key_list[1], (N_GY, N_GX, RANK, LEAF), LEAF ** -0.5, 0.375, ((0, 32), (1, 16)))
    transfer = noise(key_list[2], (LEVELS, N_GY, N_GX, RANK, 2 * RANK), (2 * RANK) ** -0.5, 0.25, ((1, 32), (2, 16)))
    coeff_out = noise(key_list[3], (N_GY, N_GX, LEAF, RANK), RANK ** -0.5, 0.375, ((0, 32), (1, 16)))
    return {"sources": sources, "coeff_in": coeff_in, "transfer": transfer, "coeff_out": coeff_out}


def apply_level(state, weights, level_bit):
    total = state.shape[0]
    block = 1 << level_bit
    groups = total // (2 * block)
    rank_rows = state.shape[1]
    cols_count = state.shape[2]
    shaped = state.reshape(groups, 2, block, rank_rows, cols_count)
    paired = jnp.concatenate([shaped[:, 0], shaped[:, 1]], axis=-2)
    paired = paired.reshape(groups * block, 2 * rank_rows, cols_count)
    wshape = weights.reshape(groups, 2, block, rank_rows, 2 * rank_rows)
    wshape = jnp.transpose(wshape, (0, 2, 1, 3, 4)).reshape(groups * block, 2 * rank_rows, 2 * rank_rows)

    def one_pair(items):
        return jnp.dot(items[0], items[1], preferred_element_type=jnp.float32).astype(jnp.bfloat16)

    result = lax.map(one_pair, (wshape, paired))
    result = result.reshape(groups, block, 2, rank_rows, cols_count)
    result = jnp.transpose(result, (0, 2, 1, 3, 4))
    return result.reshape(total, rank_rows, cols_count)


def reference(sources, coeff_in, transfer, coeff_out):
    total = N_GX * N_GY
    nbits = total.bit_length() - 1
    leaf_rows = sources.shape[2]
    cols_count = sources.shape[3]
    rank_rows = coeff_in.shape[2]
    source_flat = sources.reshape(total, leaf_rows, cols_count).astype(jnp.bfloat16)
    inward = coeff_in.reshape(total, rank_rows, leaf_rows)

    def compress(items):
        return jnp.dot(items[0], items[1], preferred_element_type=jnp.float32).astype(jnp.bfloat16)

    state = lax.map(compress, (inward, source_flat))
    for level in range(LEVELS):
        level_bit = nbits - 1 - (level % nbits)
        weights = transfer[level].reshape(total, rank_rows, 2 * rank_rows)
        state = apply_level(state, weights, level_bit)
    outward = coeff_out.reshape(total, leaf_rows, rank_rows)

    def expand(items):
        return jnp.dot(items[0], items[1], preferred_element_type=jnp.float32)

    result = lax.map(expand, (outward, state))
    return result.reshape(N_GY, N_GX, leaf_rows, cols_count)
```

```python
import jax
import jax.numpy as jnp
from jax import lax
from jax.sharding import PartitionSpec as P


LEVELS = 8
RING = 16
HOP = 4
FAR = 1
CHUNKS = 2


def swapped(value, axis, bit):
    mask = 2**bit
    pairs = [(source, source ^ mask) for source in range(lax.axis_size(axis))]
    return lax.ppermute(value, axis, pairs)


def shifted(value, step):
    pairs = [
        (source, source // RING * RING + (source + step) % RING)
        for source in range(lax.axis_size("gy"))
    ]
    return lax.ppermute(value, "gy", pairs)


def partner(state, level_bit, low_bits):
    if level_bit < low_bits:
        return swapped(state, "gx", level_bit)
    return swapped(state, "gy", level_bit - low_bits)


def dot(a, b):
    return jnp.dot(a, b, preferred_element_type=jnp.float32)


def combine(own, other, weights, upper):
    rank_rows = own.shape[0]
    lower_part = jnp.where(upper, other, own)
    upper_part = jnp.where(upper, own, other)
    total = dot(weights[:, :rank_rows], lower_part) + dot(weights[:, rank_rows:], upper_part)
    return total.astype(jnp.bfloat16)


def body(sources, coeff_in, transfer, coeff_out):
    size = lax.axis_size("gx")
    low_bits = size.bit_length() - 1
    nbits = low_bits + lax.axis_size("gy").bit_length() - 1
    position = lax.axis_index("gy") * size + lax.axis_index("gx")

    def upper_at(level):
        return position >> (nbits - 1 - level) & 1 == 1

    def exchange(state, level):
        other = partner(state, nbits - 1 - level, low_bits)
        return combine(state, other, transfer[level, 0, 0], upper_at(level))

    far_weights = partner(transfer[FAR, 0, 0], nbits - 1 - (FAR + 1), low_bits)
    state = dot(coeff_in[0, 0], sources[0, 0].astype(jnp.bfloat16)).astype(jnp.bfloat16)
    width = state.shape[1] // CHUNKS
    chunks = [state[:, k * width : (k + 1) * width] for k in range(CHUNKS)]
    others = []
    for k in range(CHUNKS):
        others.append(partner(chunks[k], nbits - 1, low_bits))
    chunks = [combine(c, o, transfer[0, 0, 0], upper_at(0)) for c, o in zip(chunks, others)]
    half = width // 2
    hops = [(shifted(c, -HOP), shifted(c, HOP)) for c in chunks]
    results = []
    for own, (after, before) in zip(chunks, hops):
        far = jnp.concatenate(
            [shifted(after[:, :half], -HOP), shifted(before[:, half:], HOP)], axis=1
        )
        near_upper = upper_at(FAR + 1)
        near = jnp.where(near_upper, before, after)
        near_far = jnp.where(near_upper, after, before)
        near = combine(near, near_far, far_weights, upper_at(FAR))
        own = combine(own, far, transfer[FAR, 0, 0], upper_at(FAR))
        results.append(combine(own, near, transfer[FAR + 1, 0, 0], near_upper))
    chunks = results
    for level in range(FAR + 2, LEVELS):
        chunks = [exchange(c, level) for c in chunks]
    state = jnp.concatenate(chunks, axis=1)
    return dot(coeff_out[0, 0], state)[None, None]


def solution(mesh):
    placed = (
        P("gy", "gx", None, None),
        P("gy", "gx", None, None),
        P(None, "gy", "gx", None, None),
        P("gy", "gx", None, None),
    )

    return jax.shard_map(
        body, mesh=mesh, in_specs=placed, out_specs=P("gy", "gx", None, None), check_vma=False
    )
```

```python
import jax
import jax.numpy as jnp
from jax import lax
from jax.experimental import pallas as pl
from jax.experimental.pallas import tpu as pltpu
from jax.sharding import PartitionSpec as P


LEVELS = 8
RING = 16
HOP = 4
FAR = 1
CHUNKS = 2
BLOCK = 256
FINISH_BYTES = 8 * 1024 * 1024


def swapped(value, axis, bit):
    mask = 2**bit
    pairs = [(source, source ^ mask) for source in range(lax.axis_size(axis))]
    return lax.ppermute(value, axis, pairs)


def shifted(value, step):
    pairs = [
        (source, source // RING * RING + (source + step) % RING)
        for source in range(lax.axis_size("gy"))
    ]
    return lax.ppermute(value, "gy", pairs)


def partner(state, level_bit, low_bits):
    if level_bit < low_bits:
        return swapped(state, "gx", level_bit)
    return swapped(state, "gy", level_bit - low_bits)


def dot(a, b):
    return jnp.dot(a, b, preferred_element_type=jnp.float32)


def combine(own, other, weights, upper):
    rank_rows = own.shape[0]
    lower_part = jnp.where(upper, other, own)
    upper_part = jnp.where(upper, own, other)
    total = dot(weights[:, :rank_rows], lower_part) + dot(weights[:, rank_rows:], upper_part)
    return total.astype(jnp.bfloat16)


def finish_kernel(flag_ref, w_ref, c_ref, own_ref, other_ref, *refs):
    out_ref, state_ref = refs[-2:]
    rank = own_ref.shape[0]
    width = out_ref.shape[1]
    left, right = w_ref[:, :rank], w_ref[:, rank:]
    here = pl.ds(pl.multiple_of(pl.program_id(0) * width, width), width)
    own, other = own_ref[:, here], other_ref[:, here]

    @pl.when(flag_ref[0] == 0)
    def _():
        total = dot(left, own) + dot(right, other)
        state_ref[...] = total.astype(jnp.bfloat16)

    @pl.when(flag_ref[0] != 0)
    def _():
        total = dot(left, other) + dot(right, own)
        state_ref[...] = total.astype(jnp.bfloat16)

    out_ref[...] = dot(c_ref[...], state_ref[...])


def finish(flag, weights, coeff, own, other, held, begin, cols):
    rank, width = own.shape
    rows = coeff.shape[0]
    block = min(width, BLOCK)
    inputs = [flag, weights, coeff, own, other]
    specs = [
        pl.BlockSpec(memory_space=pltpu.SMEM),
        pl.BlockSpec(memory_space=pltpu.VMEM),
        pl.BlockSpec(memory_space=pltpu.VMEM),
        pl.BlockSpec(memory_space=pltpu.VMEM),
        pl.BlockSpec(memory_space=pltpu.VMEM),
    ]
    aliases = {}
    if held is not None:
        inputs.append(held)
        specs.append(pl.BlockSpec(memory_space=pl.ANY))
        aliases = {5: 0}
    return pl.pallas_call(
        finish_kernel,
        grid=(width // block,),
        in_specs=specs,
        out_specs=pl.BlockSpec((rows, block), lambda i: (0, begin // block + i)),
        out_shape=jax.ShapeDtypeStruct((rows, cols), jnp.float32),
        scratch_shapes=[pltpu.VMEM((rank, block), jnp.bfloat16)],
        input_output_aliases=aliases,
        compiler_params=pltpu.CompilerParams(vmem_limit_bytes=FINISH_BYTES),
        cost_estimate=pl.CostEstimate(
            flops=2 * rank * width * (2 * rank + rows),
            bytes_accessed=4 * rows * width,
            transcendentals=0,
        ),
    )(*inputs)


def body(sources, coeff_in, transfer, coeff_out):
    size = lax.axis_size("gx")
    low_bits = size.bit_length() - 1
    nbits = low_bits + lax.axis_size("gy").bit_length() - 1
    position = lax.axis_index("gy") * size + lax.axis_index("gx")

    def upper_at(level):
        return position >> (nbits - 1 - level) & 1 == 1

    far_weights = partner(transfer[FAR, 0, 0], nbits - 1 - (FAR + 1), low_bits)
    state = dot(coeff_in[0, 0], sources[0, 0].astype(jnp.bfloat16)).astype(jnp.bfloat16)
    width = state.shape[1] // CHUNKS
    chunks = [state[:, k * width : (k + 1) * width] for k in range(CHUNKS)]
    others = []
    for k in range(CHUNKS):
        others.append(partner(chunks[k], nbits - 1, low_bits))
    chunks = [combine(c, o, transfer[0, 0, 0], upper_at(0)) for c, o in zip(chunks, others)]
    half = width // 2
    hops = []
    for chunk in chunks:
        after = shifted(chunk, -HOP)
        before = shifted(chunk, HOP)
        hops.append((after, before))
    near_upper = upper_at(FAR + 1)
    results = []
    for own, (after, before) in zip(chunks, hops):
        ahead = shifted(after[:, :half], -HOP)
        behind = shifted(before[:, half:], HOP)
        far = jnp.concatenate([ahead, behind], axis=1)
        own = combine(own, far, transfer[FAR, 0, 0], upper_at(FAR))
        near = jnp.where(near_upper, before, after)
        near_far = jnp.where(near_upper, after, before)
        near = combine(near, near_far, far_weights, upper_at(FAR))
        results.append(combine(own, near, transfer[FAR + 1, 0, 0], near_upper))
    chunks = results
    for level in range(FAR + 2, LEVELS - 1):
        others = []
        for k in range(CHUNKS):
            others.append(partner(chunks[k], nbits - 1 - level, low_bits))
        chunks = [
            combine(c, o, transfer[level, 0, 0], upper_at(level)) for c, o in zip(chunks, others)
        ]
    level = LEVELS - 1
    flag = upper_at(level).astype(jnp.int32).reshape(1)
    others = [partner(c, nbits - 1 - level, low_bits) for c in chunks]
    result = None
    for k in range(CHUNKS):
        result = finish(
            flag, transfer[level, 0, 0], coeff_out[0, 0], chunks[k], others[k],
            result, k * width, CHUNKS * width,
        )
    return result[None, None]


def solution(mesh):
    placed = (
        P("gy", "gx", None, None),
        P("gy", "gx", None, None),
        P(None, "gy", "gx", None, None),
        P("gy", "gx", None, None),
    )

    return jax.shard_map(
        body, mesh=mesh, in_specs=placed, out_specs=P("gy", "gx", None, None), check_vma=False
    )
```
